32 devices in a mesh: section: 8 (over y, x, core), tp: 4 (over z).
Axes of the slice: x: 2, y: 2, z: 4, core: 2. Of those that a mesh axis runs over, the one named last changes fastest.
Arguments:
- tokens_in: bfloat16 [2, 224, 7168], P(None, None, 'tp'), may hold values from -6 to 6
- norm_gain: float32 [2, 7168], P(None, 'tp'), may hold values from 0.5 to 2
- router_weight: float32 [2, 7168], P(None, 'tp'), may hold values from -0.0625 to 0.0625
- gate_weight: bfloat16 [8, 7168, 4608], P('section', 'tp'), may hold values from -0.0625 to 0.0625
- up_weight: bfloat16 [8, 7168, 4608], P('section', 'tp'), may hold values from -0.0625 to 0.0625
- down_weight: bfloat16 [8, 4608, 7168], P('section', None, 'tp'), may hold values from -0.046875 to 0.046875
- routed_rows: int32 [2, 2, 112], replicated, may hold values from 0 to 223, as said below
- routed_count: int32 [2, 2], replicated, may hold values from 56 to 112, as said below
Outputs:
- tokens_out: bfloat16 [2, 224, 7168], P(None, 'section', 'tp')
The draws below stay inside these ranges and needn't reach their ends.
Inputs may be any that keep to these rules, and one draw needn't show every extreme that they name: `routed_rows`: within each microbatch and layer, the 112 entries are distinct token positions. Only the leading routed_count entries of a list are live; some list is full in every draw.
All inputs are finite; a program needn't handle non-finite values.
Results may differ from the reference program's by a relative error of at most 0.0074.
Values may be sent and summed in bfloat16 or wider, within the bound.
No kernel may reach another device: no remote copies, remote signals or barrier semaphores. Data moves between devices by JAX's collectives and lax.ppermute only.
A program may use at most 128 MiB of HBM per device.

```python
import math
import jax
import jax.numpy as jnp
from jax import lax

D = 7168
FF = 18432
MB_TOKENS = 224
MICRO = 2
LAYERS = 2
HIDDEN_PARTS = 4
CAPACITY = 112


def draw_routed_rows(key, part):
    subkeys = jax.random.split(jax.random.fold_in(key, 11), MICRO * LAYERS)
    orders = jax.vmap(lambda subkey: jax.random.permutation(subkey, MB_TOKENS))(subkeys)
    return orders[:, :CAPACITY].reshape(MICRO, LAYERS, CAPACITY).astype(jnp.int32)


def draw_routed_count(key, part):
    drawn = jax.random.randint(jax.random.fold_in(key, 21), (MICRO * LAYERS,), CAPACITY // 2, CAPACITY + 1)
    position = jax.random.randint(jax.random.fold_in(key, 22), (), 0, MICRO * LAYERS)
    flattened = jnp.where(jnp.arange(MICRO * LAYERS) == position, CAPACITY, drawn)
    return flattened.reshape(MICRO, LAYERS).astype(jnp.int32)


def levels(own_key, dims, shards, smallest, top_value):
    def one(dim, parts):
        heights = jax.random.uniform(jax.random.fold_in(jax.random.fold_in(own_key, 6), dim), (parts,), jnp.float32, smallest / len(shards), top_value / len(shards))
        return jnp.repeat(jnp.exp(heights), dims[dim] // parts).reshape((-1,) + (1,) * (len(dims) - dim - 1))

    level = one(*shards[0])
    for cut in shards[1:]:
        level = level * one(*cut)
    return level


def noise(key, extent, scale, most, cuts=(), held_as=jnp.bfloat16):
    result = scale * jax.random.normal(key, extent, jnp.float32)
    if cuts:
        result = result * levels(key, extent, cuts, -0.22, 0.18)
    return jnp.clip(result, -most, most).astype(held_as)


def setup_inputs(seed: int = 0) -> dict:
    streams_of = jax.random.split(jax.random.key(seed), 9)
    tokens_in = noise(streams_of[0], (MICRO, MB_TOKENS, D), 1.0, 6.0, ((2, 4),))
    norm_gain = jnp.clip(jnp.exp(math.log(2.0) - 1.3862944 * jax.random.uniform(streams_of[1], (LAYERS, D), jnp.float32) ** levels(streams_of[1], (LAYERS, D), ((1, 4),), -0.2, 0.2)), 0.5, 2.0)
    router_weight = noise(streams_of[2], (LAYERS, D), D ** -0.5, 0.0625, ((1, 4),), jnp.float32)
    gate_weight = noise(streams_of[3], (LAYERS * HIDDEN_PARTS, D, FF // HIDDEN_PARTS), D ** -0.5, 0.0625, ((0, 8), (1, 4)))
    up_weight = noise(streams_of[4], (LAYERS * HIDDEN_PARTS, D, FF // HIDDEN_PARTS), D ** -0.5, 0.0625, ((0, 8), (1, 4)))
    down_weight = noise(streams_of[5], (LAYERS * HIDDEN_PARTS, FF // HIDDEN_PARTS, D), FF ** -0.5, 0.046875, ((0, 8), (2, 4)))
    routed_rows = draw_routed_rows(jax.random.fold_in(streams_of[8], 71), 0)
    routed_count = draw_routed_count(jax.random.fold_in(streams_of[8], 71), 0)
    return {"tokens_in": tokens_in, "norm_gain": norm_gain, "router_weight": router_weight, "gate_weight": gate_weight, "up_weight": up_weight, "down_weight": down_weight, "routed_rows": routed_rows, "routed_count": routed_count}


EPSILON = 1e-06

def run_layer(stream, routed_ids, live_count, gain_row, router_row, gate_full, up_full, down_full):
    picked = stream[routed_ids]
    floats = picked.astype(jnp.float32)
    squares = lax.optimization_barrier(jnp.sum(floats * floats, axis=1))
    logits = lax.optimization_barrier(jnp.sum(floats * router_row, axis=1))
    inverse = lax.rsqrt(squares / D + EPSILON)[:, None]
    scaled = (floats * gain_row).astype(jnp.bfloat16)
    gate = jnp.dot(scaled, gate_full, preferred_element_type=jnp.float32) * inverse
    up_values = jnp.dot(scaled, up_full, preferred_element_type=jnp.float32) * inverse
    hidden = (jax.nn.silu(gate) * up_values).astype(jnp.bfloat16)
    output = jnp.dot(hidden, down_full, preferred_element_type=jnp.float32)
    router_gate = jax.nn.sigmoid(logits)[:, None]
    updated = (floats + router_gate * output).astype(jnp.bfloat16)
    is_live = jnp.arange(routed_ids.shape[0], dtype=jnp.int32) < live_count
    new_rows = jnp.where(is_live[:, None], updated, picked)
    return stream.at[routed_ids].set(new_rows)

def reference(tokens_in, norm_gain, router_weight, gate_weight, up_weight, down_weight, routed_rows, routed_count):
    streams = tokens_in
    for layer_index in range(LAYERS):
        first = layer_index * HIDDEN_PARTS
        last = first + HIDDEN_PARTS
        gate_full = jnp.transpose(gate_weight[first:last], (1, 0, 2)).reshape(D, FF)
        up_full = jnp.transpose(up_weight[first:last], (1, 0, 2)).reshape(D, FF)
        down_full = down_weight[first:last].reshape(FF, D)
        streams = jax.vmap(run_layer, in_axes=(0, 0, 0, None, None, None, None, None))(streams, routed_rows[:, layer_index], routed_count[:, layer_index], norm_gain[layer_index], router_weight[layer_index], gate_full, up_full, down_full)
    return streams
```

```python
import jax
import jax.numpy as jnp
from jax import lax
from jax.experimental import pallas as pl
from jax.experimental.pallas import tpu as pltpu
from jax.sharding import PartitionSpec as P


LAYERS = 2
EPSILON = 1e-06
LANES = 128
F32 = jnp.float32
BF16 = jnp.bfloat16


def swapped(value, axis, mask):
    pairs = [(i, i ^ mask) for i in range(lax.axis_size(axis))]
    return lax.ppermute(value, axis, pairs)


def layer_swapped(value, layer, section_mask, tp_mask):
    tp_size = lax.axis_size("tp")
    group_size = lax.axis_size("section") // LAYERS
    pairs = []
    for s in range(layer * group_size, (layer + 1) * group_size):
        for t in range(tp_size):
            pairs.append((s * tp_size + t, (s ^ section_mask) * tp_size + (t ^ tp_mask)))
    return lax.ppermute(value, ("section", "tp"), pairs)


def sent_to_others(value, layer):
    tp_size = lax.axis_size("tp")
    group_size = lax.axis_size("section") // LAYERS
    pairs = []
    for s in range(layer * group_size, (layer + 1) * group_size):
        for t in range(tp_size):
            pairs.append((s * tp_size + t, (s ^ group_size) * tp_size + t))
    return lax.ppermute(value, ("section", "tp"), pairs)


def row_cuts(rows):
    helped = rows * 2 // 7 // 16 * 16
    first = ((rows - helped) // 2 + 15) // 16 * 16
    return [(0, first), (first, rows - helped), (rows - helped, rows)]


def in_hbm(value):
    return pltpu.with_memory_space_constraint(value, pltpu.HBM)


def block_of(extent, most, step):
    best = step
    for size in range(step, min(extent, most) + 1, step):
        if extent % size == 0:
            best = size
    return best


def front_half(scaled, gate_block, up_block, half, active, cuts):
    rows, depth = scaled.shape
    width = gate_block.shape[1] // 2
    if width % LANES:
        picked = [lax.dynamic_slice_in_dim(w, half * width, width, 1) for w in (gate_block, up_block)]
        both = jnp.stack([jnp.dot(scaled, w, preferred_element_type=F32).astype(BF16) for w in picked])
        return [both[:, lo:hi] for lo, hi in cuts]
    cols = block_of(width, 768, LANES)
    steps = width // cols

    def kernel(half_ref, x_ref, g_ref, u_ref, *o_refs):
        @pl.when(half_ref[1] == 1)
        def _():
            x = x_ref[...]
            for i, w_ref in enumerate((g_ref, u_ref)):
                product = jnp.dot(x, w_ref[...], preferred_element_type=F32).astype(BF16)
                for (lo, hi), o_ref in zip(cuts, o_refs):
                    o_ref[i] = product[lo:hi]

    weight_spec = pl.BlockSpec((depth, cols), lambda i, h: (0, (h[0] * steps + i) * h[1]))
    return pl.pallas_call(
        kernel,
        out_shape=[jax.ShapeDtypeStruct((2, hi - lo, width), BF16) for lo, hi in cuts],
        grid_spec=pltpu.PrefetchScalarGridSpec(
            num_scalar_prefetch=1,
            grid=(steps,),
            in_specs=[pl.BlockSpec((rows, depth), lambda i, h: (0, 0)), weight_spec, weight_spec],
            out_specs=[pl.BlockSpec((2, hi - lo, cols), lambda i, h: (0, 0, i)) for lo, hi in cuts],
        ),
        cost_estimate=pl.CostEstimate(
            flops=4 * rows * depth * width, bytes_accessed=4 * depth * width, transcendentals=0
        ),
        compiler_params=pltpu.CompilerParams(vmem_limit_bytes=32 * 2**20),
        name="front_half",
    )(jnp.stack([half, active]), scaled, in_hbm(gate_block), in_hbm(up_block))


def back_half(hidden, down_block, half, side, active, base=None):
    rows, depth = hidden.shape
    cols = down_block.shape[1] // 2
    if depth % LANES or cols % LANES:
        results = []
        for i in range(2):
            column = (1 - side if i == 0 else side) * cols
            picked = lax.dynamic_slice(down_block, (half * depth, column), (depth, cols))
            result = jnp.dot(hidden, picked, preferred_element_type=F32)
            results.append(result if base is None else result + base[i].astype(F32))
        return results[0] if base is None else results[0].astype(BF16), results[1]
    held_as = (F32, F32) if base is None else (BF16, F32)

    def kernel(half_ref, x_ref, w_ref, *refs):
        for i, o_ref in enumerate(refs[-2:]):

            @pl.when((pl.program_id(0) == i) & (half_ref[2] == 1))
            def _():
                product = jnp.dot(x_ref[...], w_ref[...], preferred_element_type=F32)
                if base is not None:
                    product = product + refs[i][...]
                o_ref[...] = product.astype(held_as[i])

    whole = pl.BlockSpec((rows, cols), lambda i, h: (0, 0))
    in_specs = [
        pl.BlockSpec((rows, depth), lambda i, h: (0, 0)),
        pl.BlockSpec((depth, cols), lambda i, h: (h[0] * h[2], jnp.where(i == h[2], h[1], 1 - h[1]))),
    ]
    operands = [hidden, in_hbm(down_block)]
    if base is not None:
        in_specs += [whole, whole]
        operands += list(base)
    return pl.pallas_call(
        kernel,
        out_shape=[jax.ShapeDtypeStruct((rows, cols), t) for t in held_as],
        grid_spec=pltpu.PrefetchScalarGridSpec(
            num_scalar_prefetch=1, grid=(2,), in_specs=in_specs, out_specs=[whole, whole]
        ),
        cost_estimate=pl.CostEstimate(
            flops=4 * rows * depth * cols, bytes_accessed=4 * depth * cols, transcendentals=0
        ),
        compiler_params=pltpu.CompilerParams(vmem_limit_bytes=32 * 2**20),
        name="back_half",
    )(jnp.stack([half, side, active]), *operands)


def joined(own, other, upper):
    return jnp.where(
        upper, jnp.concatenate([other, own], axis=-1), jnp.concatenate([own, other], axis=-1)
    )


def on_device(
    tokens_in,
    norm_gain,
    router_weight,
    gate_weight,
    up_weight,
    down_weight,
    routed_rows,
    routed_count,
):
    micro_count, token_count, quarter = tokens_in.shape
    capacity = routed_rows.shape[2]
    model_width = quarter * lax.axis_size("tp")
    section_index = lax.axis_index("section")
    section_size = lax.axis_size("section")
    group_size = section_size // LAYERS
    layer_index = section_index // group_size
    tp_index = lax.axis_index("tp")
    tp_bits = lax.axis_size("tp").bit_length() - 1
    gate_block = gate_weight[0]
    up_block = up_weight[0]
    down_block = down_weight[0]
    pair_bit = (tp_index % 2).astype(jnp.int32)
    core_bit = section_index % 2

    def summed_over_tp(value):
        for bit in range(tp_bits):
            other = swapped(value, "tp", 2**bit)
            value = value + other
        return value

    def row_sums(picked, k):
        floats = picked.astype(F32)
        return jnp.stack([jnp.sum(floats * floats, axis=1), jnp.sum(floats * router_weight[k], axis=1)])

    def cross_sums(parts, plane):
        for bit in range(1, tp_bits):
            width = parts[0].shape[2] // 2
            side = tp_index // 2**bit % 2
            give = sum(
                lax.dynamic_slice_in_dim(p, (1 - side) * width, width, 2).astype(F32) for p in parts
            ).astype(BF16)
            parts = [lax.dynamic_slice_in_dim(p, side * width, width, 2) for p in parts]
            parts.append(layer_swapped(give, plane, 0, 2**bit))
        return parts

    def hidden_halves(parts, inverse, plane):
        total = sum(p.astype(F32) for p in parts)
        gate = total[0] * inverse
        hidden = (jax.nn.silu(gate) * (total[1] * inverse)).astype(BF16)
        for bit in reversed(range(1, tp_bits)):
            upper = tp_index // 2**bit % 2 == 1
            other = layer_swapped(hidden, plane, 0, 2**bit)
            hidden = joined(hidden, other, upper)
        return hidden, layer_swapped(hidden, plane, 0, 1)

    def layer_output(picked, squares, k):
        on_layer = layer_index == k
        active = on_layer.astype(jnp.int32)
        helper = LAYERS - 1 - k
        cuts = row_cuts(picked.shape[0])
        planes = (k, k, helper)
        scaled = (picked.astype(F32) * norm_gain[k]).astype(BF16)
        inverse = lax.rsqrt(squares / model_width + EPSILON)[:, None]
        given = list(front_half(scaled, gate_block, up_block, 1 - pair_bit, active, cuts))
        given[2] = sent_to_others(given[2], k)
        kept = list(front_half(scaled, gate_block, up_block, pair_bit, active, cuts))
        kept[2] = sent_to_others(kept[2], k)
        halves = []
        for i, (lo, hi) in enumerate(cuts):
            received = layer_swapped(given[i], planes[i], 0, 1)
            parts = cross_sums([kept[i], received], planes[i])
            halves.append(hidden_halves(parts, inverse[lo:hi], planes[i]))
        own_h = sent_to_others(halves[2][0], helper)
        other_h = sent_to_others(halves[2][1], helper)
        own = jnp.concatenate([halves[0][0], halves[1][0], own_h])
        other = jnp.concatenate([halves[0][1], halves[1][1], other_h])
        base = back_half(own, down_block, pair_bit, core_bit, active)
        give, keep = back_half(other, down_block, 1 - pair_bit, core_bit, active, base)
        got = layer_swapped(give, k, 1, 0)
        piece = (keep + got.astype(F32)).astype(BF16)
        middle = piece.shape[0] // 2
        bits = [2**b for b in range(1, group_size.bit_length() - 1)]
        one = sent_to_others(piece[:middle], k)
        one = jnp.where(on_layer, piece[:middle], one)
        two = piece[middle:]
        for bit in bits:
            got = layer_swapped(two, k, bit, 0)
            two = (two.astype(F32) + got.astype(F32)).astype(BF16)
        for bit in bits:
            got = swapped(one, "section", bit)
            one = (one.astype(F32) + got.astype(F32)).astype(BF16)
        got = sent_to_others(two, k)
        two = jnp.where(on_layer, two, got)
        upper = core_bit == 1
        return jnp.concatenate(
            [joined(v, swapped(v, "section", 1), upper) for v in (one, two)]
        )

    def places(ids, wanted):
        same = wanted[:, None] == ids[None, :]
        at = jnp.sum(jnp.where(same, jnp.arange(ids.shape[0], dtype=jnp.int32)[None, :], 0), axis=1)
        return jnp.any(same, axis=1)[:, None], at

    def taken(source, at):
        return jnp.take(source, at, axis=0, mode="clip")

    rows_all = micro_count * capacity
    stream = tokens_in.reshape(micro_count * token_count, quarter)
    first_token = jnp.arange(micro_count, dtype=jnp.int32)[:, None] * token_count
    span = token_count // section_size
    held = (first_token + section_index * span + jnp.arange(span, dtype=jnp.int32)).reshape(-1)
    result = lax.dynamic_slice_in_dim(tokens_in, section_index * span, span, 1)
    result = result.reshape(micro_count * span, quarter)
    done = []
    for k in range(LAYERS):
        ids = (routed_rows[:, k] + first_token).reshape(rows_all)
        live = jnp.arange(capacity, dtype=jnp.int32)[None] < routed_count[:, k][:, None]
        picked = taken(stream, ids)
        for earlier_ids, earlier_rows in done:
            found, at = places(earlier_ids, ids)
            picked = jnp.where(found, taken(earlier_rows, at), picked)
        sums = summed_over_tp(row_sums(picked, k))
        output = layer_output(picked, sums[0], k)
        router_gate = jax.nn.sigmoid(sums[1])[:, None]
        updated = (picked.astype(F32) + router_gate * output.astype(F32)).astype(BF16)
        rows = jnp.where(live.reshape(rows_all, 1), updated, picked)
        done.append((ids, rows))
        found, at = places(ids, held)
        result = jnp.where(found, taken(rows, at), result)
    return result.reshape(micro_count, span, quarter)


def solution(mesh):
    return jax.shard_map(
        on_device,
        mesh=mesh,
        in_specs=(
            P(None, None, "tp"),
            P(None, "tp"),
            P(None, "tp"),
            P("section", "tp", None),
            P("section", "tp", None),
            P("section", None, "tp"),
            P(),
            P(),
        ),
        out_specs=P(None, "section", "tp"),
        check_vma=False,
    )
```

```python
import jax
import jax.numpy as jnp
from jax import lax
from jax.experimental import pallas as pl
from jax.experimental.pallas import tpu as pltpu
from jax.sharding import PartitionSpec as P


LAYERS = 2
EPSILON = 1e-06
LANES = 128
F32 = jnp.float32
BF16 = jnp.bfloat16


def swapped(value, axis, mask):
    pairs = [(i, i ^ mask) for i in range(lax.axis_size(axis))]
    return lax.ppermute(value, axis, pairs)


def layer_swapped(value, layer, section_mask, tp_mask):
    tp_size = lax.axis_size("tp")
    group_size = lax.axis_size("section") // LAYERS
    pairs = []
    for s in range(layer * group_size, (layer + 1) * group_size):
        for t in range(tp_size):
            pairs.append((s * tp_size + t, (s ^ section_mask) * tp_size + (t ^ tp_mask)))
    return lax.ppermute(value, ("section", "tp"), pairs)


def sent_to_others(value, layer):
    tp_size = lax.axis_size("tp")
    group_size = lax.axis_size("section") // LAYERS
    pairs = []
    for s in range(layer * group_size, (layer + 1) * group_size):
        for t in range(tp_size):
            pairs.append((s * tp_size + t, (s ^ group_size) * tp_size + t))
    return lax.ppermute(value, ("section", "tp"), pairs)


def row_cuts(rows):
    tile = 16
    helped = rows * 2 // 7 // tile * tile
    kept = rows - helped
    edge = kept // 3 // tile * tile
    marks = [0, edge, kept - edge, kept, rows]
    return list(zip(marks, marks[1:]))


def block_of(extent, most, step):
    best = step
    for size in range(step, min(extent, most) + 1, step):
        if extent % size == 0:
            best = size
    return best


def front_half(scaled, gate_block, up_block, half, active, cuts):
    rows, depth = scaled.shape
    width = gate_block.shape[1] // 2
    if width % LANES:
        picked = [lax.dynamic_slice_in_dim(w, half * width, width, 1) for w in (gate_block, up_block)]
        both = jnp.stack([jnp.dot(scaled, w, preferred_element_type=F32).astype(BF16) for w in picked])
        return [both[:, lo:hi] for lo, hi in cuts]
    cols = block_of(width, 2 * LANES, LANES)
    steps = width // cols

    def kernel(half_ref, x_ref, g_ref, u_ref, *refs):
        o_refs, w_ref, done = refs[: len(cuts)], refs[-2], refs[-1]

        def copy(j, i):
            start = pl.multiple_of(half_ref[0] * width + j * cols, LANES)
            source = (g_ref, u_ref)[i].at[:, pl.ds(start, cols)]
            return pltpu.make_async_copy(source, w_ref.at[j, i], done.at[j, i])

        @pl.when(half_ref[1] == 1)
        def _():
            def start(j, carried):
                copy(j, 0).start()
                copy(j, 1).start()
                return carried

            lax.fori_loop(0, steps, start, 0)

            def multiply(j, carried):
                column = pl.multiple_of(j * cols, LANES)
                copy(j, 0).wait()
                copy(j, 1).wait()
                x = x_ref[...]
                products = [jnp.dot(x, w_ref[j, i], preferred_element_type=F32) for i in range(2)]
                for i, product in enumerate(products):
                    for (lo, hi), o_ref in zip(cuts, o_refs):
                        o_ref[i, :, pl.ds(column, cols)] = product[lo:hi].astype(BF16)
                return carried

            lax.fori_loop(0, steps, multiply, 0)

    return pl.pallas_call(
        kernel,
        out_shape=[jax.ShapeDtypeStruct((2, hi - lo, width), BF16) for lo, hi in cuts],
        in_specs=[
            pl.BlockSpec(memory_space=pltpu.SMEM),
            pl.BlockSpec(memory_space=pltpu.VMEM),
            pl.BlockSpec(memory_space=pltpu.HBM),
            pl.BlockSpec(memory_space=pltpu.HBM),
        ],
        out_specs=[pl.BlockSpec(memory_space=pltpu.VMEM) for _ in cuts],
        scratch_shapes=[
            pltpu.VMEM((steps, 2, depth, cols), BF16),
            pltpu.SemaphoreType.DMA((steps, 2)),
        ],
        cost_estimate=pl.CostEstimate(
            flops=4 * rows * depth * width, bytes_accessed=4 * depth * width, transcendentals=0
        ),
        compiler_params=pltpu.CompilerParams(vmem_limit_bytes=40 * 2**20),
        name="front_half",
    )(jnp.stack([half, active]), scaled, gate_block, up_block)


def back_half(hidden, down_block, half, side, active, base=None):
    rows, depth = hidden.shape
    width = down_block.shape[1]
    cols = width // 2
    held_as = F32 if base is None else BF16
    if depth % LANES or cols % LANES:
        results = []
        for i in range(2):
            column = (1 - side if i == 0 else side) * cols
            picked = lax.dynamic_slice(down_block, (half * depth, column), (depth, cols))
            results.append(jnp.dot(hidden, picked, preferred_element_type=F32))
        result = jnp.stack(results)
        return (result if base is None else result + base).astype(held_as)
    block = 2 * LANES
    steps = width // block
    per_side = cols // LANES

    def kernel(half_ref, x_ref, down_ref, *refs):
        o_ref, w_ref, done = refs[-3:]

        def copy(j):
            row = pl.multiple_of(half_ref[0] * depth, LANES)
            column = pl.multiple_of(j * block, LANES)
            source = down_ref.at[pl.ds(row, depth), pl.ds(column, block)]
            return pltpu.make_async_copy(source, w_ref.at[j], done.at[j])

        @pl.when(half_ref[2] == 1)
        def _():
            def start(j, carried):
                copy(j).start()
                return carried

            lax.fori_loop(0, steps, start, 0)

            def multiply(j, carried):
                copy(j).wait()
                product = jnp.dot(x_ref[...], w_ref[j], preferred_element_type=F32)
                for i in range(2):
                    piece = 2 * j + i
                    place = jnp.where(piece >= per_side, 1, 0)
                    column = pl.multiple_of((piece - place * per_side) * LANES, LANES)
                    place = jnp.where(place == half_ref[1], 1, 0)
                    value = product[:, i * LANES : (i + 1) * LANES]
                    if base is not None:
                        value = value + refs[0][place, :, pl.ds(column, LANES)]
                    o_ref[place, :, pl.ds(column, LANES)] = value.astype(held_as)
                return carried

            lax.fori_loop(0, steps, multiply, 0)

    return pl.pallas_call(
        kernel,
        out_shape=jax.ShapeDtypeStruct((2, rows, cols), held_as),
        in_specs=[
            pl.BlockSpec(memory_space=pltpu.SMEM),
            pl.BlockSpec(memory_space=pltpu.VMEM),
            pl.BlockSpec(memory_space=pltpu.HBM),
        ]
        + ([] if base is None else [pl.BlockSpec(memory_space=pltpu.VMEM)]),
        out_specs=pl.BlockSpec(memory_space=pltpu.VMEM),
        scratch_shapes=[pltpu.VMEM((steps, depth, block), BF16), pltpu.SemaphoreType.DMA((steps,))],
        cost_estimate=pl.CostEstimate(
            flops=2 * rows * depth * width, bytes_accessed=2 * depth * width, transcendentals=0
        ),
        compiler_params=pltpu.CompilerParams(vmem_limit_bytes=40 * 2**20),
        name="back_half",
    )(jnp.stack([half, side, active]), hidden, down_block, *([] if base is None else [base]))


def joined(own, other, upper):
    return jnp.where(
        upper, jnp.concatenate([other, own], axis=-1), jnp.concatenate([own, other], axis=-1)
    )


def on_device(
    tokens_in,
    norm_gain,
    router_weight,
    gate_weight,
    up_weight,
    down_weight,
    routed_rows,
    routed_count,
):
    micro_count, token_count, quarter = tokens_in.shape
    capacity = routed_rows.shape[2]
    model_width = quarter * lax.axis_size("tp")
    section_index = lax.axis_index("section")
    section_size = lax.axis_size("section")
    group_size = section_size // LAYERS
    layer_index = section_index // group_size
    tp_index = lax.axis_index("tp")
    tp_bits = lax.axis_size("tp").bit_length() - 1
    gate_block = gate_weight[0]
    up_block = up_weight[0]
    down_block = down_weight[0]
    pair_bit = (tp_index % 2).astype(jnp.int32)
    core_bit = section_index % 2

    def summed_over_tp(value):
        for bit in range(tp_bits):
            other = swapped(value, "tp", 2**bit)
            value = value + other
        return value

    def row_sums(picked, k):
        floats = picked.astype(F32)
        return jnp.stack([jnp.sum(floats * floats, axis=1), jnp.sum(floats * router_weight[k], axis=1)])

    def cross_sums(parts, plane):
        for bit in range(1, tp_bits):
            width = parts[0].shape[2] // 2
            side = tp_index // 2**bit % 2
            give = sum(
                lax.dynamic_slice_in_dim(p, (1 - side) * width, width, 2).astype(F32) for p in parts
            ).astype(BF16)
            parts = [lax.dynamic_slice_in_dim(p, side * width, width, 2) for p in parts]
            parts.append(layer_swapped(give, plane, 0, 2**bit))
        return parts

    def hidden_halves(parts, inverse, plane):
        total = sum(p.astype(F32) for p in parts)
        gate = total[0] * inverse
        hidden = (jax.nn.silu(gate) * (total[1] * inverse)).astype(BF16)
        for bit in reversed(range(1, tp_bits)):
            upper = tp_index // 2**bit % 2 == 1
            other = layer_swapped(hidden, plane, 0, 2**bit)
            hidden = joined(hidden, other, upper)
        return hidden, layer_swapped(hidden, plane, 0, 1)

    def layer_output(picked, squares, k):
        on_layer = layer_index == k
        active = on_layer.astype(jnp.int32)
        helper = LAYERS - 1 - k
        cuts = row_cuts(picked.shape[0])
        last = len(cuts) - 1
        planes = [k] * last + [helper]
        scaled = (picked.astype(F32) * norm_gain[k]).astype(BF16)
        inverse = lax.rsqrt(squares / model_width + EPSILON)[:, None]
        given = list(front_half(scaled, gate_block, up_block, 1 - pair_bit, active, cuts))
        given[last] = sent_to_others(given[last], k)
        kept = list(front_half(scaled, gate_block, up_block, pair_bit, active, cuts))
        kept[last] = sent_to_others(kept[last], k)
        own = []
        other = []
        for i, (lo, hi) in enumerate(cuts):
            received = layer_swapped(given[i], planes[i], 0, 1)
            parts = cross_sums([kept[i], received], planes[i])
            halves = hidden_halves(parts, inverse[lo:hi], planes[i])
            own.append(halves[0])
            other.append(halves[1])
        own[last] = sent_to_others(own[last], helper)
        other[last] = sent_to_others(other[last], helper)
        own = jnp.concatenate(own)
        other = jnp.concatenate(other)
        base = back_half(own, down_block, pair_bit, core_bit, active)
        give, keep = back_half(other, down_block, 1 - pair_bit, core_bit, active, base)
        got = layer_swapped(give, k, 1, 0)
        piece = (keep.astype(F32) + got.astype(F32)).astype(BF16)
        middle = piece.shape[0] // 2
        bits = [2**b for b in range(1, group_size.bit_length() - 1)]
        one = sent_to_others(piece[:middle], k)
        two = piece[middle:]
        for bit in bits:
            got = layer_swapped(two, k, bit, 0)
            two = (two.astype(F32) + got.astype(F32)).astype(BF16)
        one = jnp.where(on_layer, lax.optimization_barrier(piece[:middle]), one)
        for bit in bits:
            got = swapped(one, "section", bit)
            one = (one.astype(F32) + got.astype(F32)).astype(BF16)
        got = sent_to_others(two, k)
        two = jnp.where(on_layer, two, got)
        upper = core_bit == 1
        return jnp.concatenate(
            [joined(v, swapped(v, "section", 1), upper) for v in (one, two)]
        )

    def overlaid(base, ids, rows, wanted):
        same = wanted[:, None] == ids[None, :]
        held_rows = jnp.dot(same.astype(BF16), rows, preferred_element_type=F32).astype(BF16)
        return jnp.where(jnp.any(same, axis=1)[:, None], held_rows, base)

    rows_all = micro_count * capacity
    stream = tokens_in.reshape(micro_count * token_count, quarter)
    first_token = jnp.arange(micro_count, dtype=jnp.int32)[:, None] * token_count
    span = token_count // section_size
    held = (first_token + section_index * span + jnp.arange(span, dtype=jnp.int32)).reshape(-1)
    result = lax.dynamic_slice_in_dim(tokens_in, section_index * span, span, 1)
    result = result.reshape(micro_count * span, quarter)
    done = []
    entering = []
    for k in range(LAYERS):
        ids = (routed_rows[:, k] + first_token).reshape(rows_all)
        entering.append(jnp.take(stream, ids, axis=0, unique_indices=True, mode="clip"))
    for k in range(LAYERS):
        ids = (routed_rows[:, k] + first_token).reshape(rows_all)
        live = jnp.arange(capacity, dtype=jnp.int32)[None] < routed_count[:, k][:, None]
        picked = entering[k]
        for earlier_ids, earlier_rows in done:
            picked = overlaid(picked, earlier_ids, earlier_rows, ids)
        sums = summed_over_tp(row_sums(picked, k))
        output = layer_output(picked, sums[0], k)
        router_gate = jax.nn.sigmoid(sums[1])[:, None]
        updated = (picked.astype(F32) + router_gate * output.astype(F32)).astype(BF16)
        rows = jnp.where(live.reshape(rows_all, 1), updated, picked)
        done.append((ids, rows))
        result = overlaid(result, ids, rows, held)
    return result.reshape(micro_count, span, quarter)


def solution(mesh):
    return jax.shard_map(
        on_device,
        mesh=mesh,
        in_specs=(
            P(None, None, "tp"),
            P(None, "tp"),
            P(None, "tp"),
            P("section", "tp", None),
            P("section", "tp", None),
            P("section", None, "tp"),
            P(),
            P(),
        ),
        out_specs=P(None, "section", "tp"),
        check_vma=False,
    )
```
